32 devices in a mesh: seq: 8 (over z, x), head: 4 (over y, core).
Axes of the slice: x: 2, y: 2, z: 4, core: 2. Of those that a mesh axis runs over, the one named last changes fastest.
Arguments:
- block_input: bfloat16 [4096, 2048], P('seq'), may hold values from -6 to 6
- out_cotangent: bfloat16 [4096, 2048], P('seq'), may hold values from -6 to 6
- decay_rate: float32 [8], P('head'), may hold values from 0 to 1, as said below
- first_scale: float32 [2048], replicated, may hold values from 0.5 to 1.5
- first_shift: float32 [2048], replicated, may hold values from -3 to 3
- query_weight: bfloat16 [2048, 2048], P(None, 'head'), may hold values from -0.125 to 0.125
- key_weight: bfloat16 [2048, 2048], P(None, 'head'), may hold values from -0.125 to 0.125
- value_weight: bfloat16 [2048, 4096], P(None, 'head'), may hold values from -0.125 to 0.125
- gate_weight: bfloat16 [2048, 4096], P(None, 'head'), may hold values from -0.125 to 0.125
- output_weight: bfloat16 [4096, 2048], P('head'), may hold values from -0.1875 to 0.1875
- second_scale: float32 [2048], replicated, may hold values from 0.5 to 1.5
- second_shift: float32 [2048], replicated, may hold values from -3 to 3
- up_weight: bfloat16 [2048, 4096], P(None, 'head'), may hold values from -0.125 to 0.125
- mlp_gate_weight: bfloat16 [2048, 4096], P(None, 'head'), may hold values from -0.125 to 0.125
- down_weight: bfloat16 [4096, 2048], P('head'), may hold values from -0.1875 to 0.1875
Outputs:
- block_output: bfloat16 [4096, 2048], P('seq')
- input_grad: bfloat16 [4096, 2048], P('seq')
- first_scale_grad: float32 [2048], P('seq')
- first_shift_grad: float32 [2048], P('seq')
- query_grad: float32 [2048, 2048], P('seq', 'head')
- key_grad: float32 [2048, 2048], P('seq', 'head')
- value_grad: float32 [2048, 4096], P('seq', 'head')
- gate_grad: float32 [2048, 4096], P('seq', 'head')
- output_grad: float32 [4096, 2048], P('head', 'seq')
- second_scale_grad: float32 [2048], P('seq')
- second_shift_grad: float32 [2048], P('seq')
- up_grad: float32 [2048, 4096], P('seq', 'head')
- mlp_gate_grad: float32 [2048, 4096], P('seq', 'head')
- down_grad: float32 [4096, 2048], P('head', 'seq')
The draws below stay inside these ranges and needn't reach their ends.
Inputs may be any that keep to these rules, and one draw needn't show every extreme that they name: `decay_rate`: every rate is positive.
All inputs are finite; a program needn't handle non-finite values.
Results may differ from the reference program's by a relative error of at most 0.015.
The reference program's roundings to bfloat16 on the way count: a program that leaves them out, or rounds other values in their place, can miss the bound.
Values sent between devices are 32-bit elements; how exact they have to be, the bound alone decides.
A program may use at most 256 MiB of HBM per device.

```python
import jax
import jax.numpy as jnp
from jax import lax

D = 2048
HEADS = 8
KD = 256
VD = 512
FF = 4096
TOK_DEV = 512
LENGTH = 4096


def draw_decay_rate(key, part):
    order_key = jax.random.fold_in(key, 11)
    slow_key = jax.random.fold_in(key, 12)
    fast_key = jax.random.fold_in(key, 13)
    head_rank = jax.random.permutation(order_key, HEADS)
    slow_count = HEADS // 2
    slow_rate = jax.random.uniform(slow_key, (HEADS,), jnp.float32, 0.2, 1.0) * (2.3 / LENGTH)
    fast_rate = 1.0 / jax.random.uniform(fast_key, (HEADS,), jnp.float32, 30.0, 50.0)
    return jnp.where(head_rank < slow_count, slow_rate, fast_rate).astype(jnp.float32)


def block_scale(own_key, extent, cuts, low, largest):
    def one(position, parts):
        draws = jax.random.uniform(jax.random.fold_in(jax.random.fold_in(own_key, 6), position), (parts,), jnp.float32, low / len(cuts), largest / len(cuts))
        return jnp.repeat(jnp.exp(draws), extent[position] // parts).reshape((-1,) + (1,) * (len(extent) - position - 1))

    factor_of = one(*cuts[0])
    for cut in cuts[1:]:
        factor_of = factor_of * one(*cut)
    return factor_of


def gaussian(stream_key, extent, deviation, bound, split=(), kind=jnp.bfloat16):
    values = deviation * jax.random.normal(stream_key, extent, jnp.float32)
    if split:
        values = values * block_scale(stream_key, extent, split, -0.22, 0.18)
    return jnp.clip(values, -bound, bound).astype(kind)


def setup_inputs(seed: int = 0) -> dict:
    splits = jax.random.split(jax.random.key(seed), 16)
    return {
        "block_input": gaussian(splits[0], (LENGTH, D), 1.0, 6.0, ((0, 8),)),
        "out_cotangent": gaussian(splits[1], (LENGTH, D), 1.0, 6.0, ((0, 8),)),
        "decay_rate": draw_decay_rate(jax.random.fold_in(splits[15], 71), 0),
        "first_scale": jnp.clip(1.0 + 0.1 * jax.random.normal(splits[3], (D,), jnp.float32), 0.5, 1.5),
        "first_shift": gaussian(splits[4], (D,), 0.5, 3.0, (), jnp.float32),
        "query_weight": gaussian(splits[5], (D, HEADS * KD), D ** -0.5, 0.125, ((1, 4),)),
        "key_weight": gaussian(splits[6], (D, HEADS * KD), D ** -0.5, 0.125, ((1, 4),)),
        "value_weight": gaussian(splits[7], (D, HEADS * VD), D ** -0.5, 0.125, ((1, 4),)),
        "gate_weight": gaussian(splits[8], (D, HEADS * VD), D ** -0.5, 0.125, ((1, 4),)),
        "output_weight": gaussian(splits[9], (HEADS * VD, D), (HEADS * VD // 4) ** -0.5, 0.1875, ((0, 4),)),
        "second_scale": jnp.clip(1.0 + 0.1 * jax.random.normal(splits[10], (D,), jnp.float32), 0.5, 1.5),
        "second_shift": gaussian(splits[11], (D,), 0.5, 3.0, (), jnp.float32),
        "up_weight": gaussian(splits[12], (D, FF), D ** -0.5, 0.125, ((1, 4),)),
        "mlp_gate_weight": gaussian(splits[13], (D, FF), D ** -0.5, 0.125, ((1, 4),)),
        "down_weight": gaussian(splits[14], (FF, D), (FF // 4) ** -0.5, 0.1875, ((0, 4),)),
    }


EPSILON = 1e-05
FULL_ACCURACY = lax.Precision.HIGHEST

def layer_norm(values, scales, shifts):
    centred = values - lax.optimization_barrier(jnp.mean(values, axis=-1, keepdims=True))
    inverse = lax.rsqrt(lax.optimization_barrier(jnp.mean(centred * centred, axis=-1, keepdims=True)) + EPSILON)
    normed = centred * inverse
    return (normed * scales + shifts, normed, inverse)

def norm_back(upstream, normed, inverse):
    return inverse * (upstream - lax.optimization_barrier(jnp.mean(upstream, axis=-1, keepdims=True)) - normed * lax.optimization_barrier(jnp.mean(upstream * normed, axis=-1, keepdims=True)))

def gelu_pair(pre_act):
    normal_cdf = 0.5 * (1.0 + lax.erf(pre_act * 0.7071067811865476))
    density = jnp.exp(-0.5 * pre_act * pre_act) * 0.3989422804014327
    return (pre_act * normal_cdf, normal_cdf + pre_act * density)

def decay_tables(decay_rates, length):
    places = jnp.arange(length, dtype=jnp.float32)
    distance = places[:, None] - places[None, :]
    causal = distance >= 0.0
    decay_mask = jnp.where(causal[None], jnp.exp(-decay_rates[:, None, None] * jnp.where(causal, distance, 0.0)[None]), 0.0)
    arriving_fading_factor = jnp.exp(-places[:, None] * decay_rates[None, :])[:, :, None]
    outgoing_decay = jnp.exp(-(length - places)[:, None] * decay_rates[None, :])[:, :, None]
    return (decay_mask, arriving_fading_factor, outgoing_decay)

def contract_rows(left_side, right_side):
    return lax.dot_general(left_side, right_side, (((0,), (0,)), ((), ())), preferred_element_type=jnp.float32)

def times_transpose(left_side, right_side):
    return lax.dot_general(left_side, right_side, (((1,), (1,)), ((), ())), preferred_element_type=jnp.float32)

def layer_block(block_piece, cot_piece, arriving_memory_matrix, state_gradient, weights, decay_rates):
    first_scale, first_shift, query_weight, key_weight, value_weight, gate_weight, output_weight, second_scale, second_shift, up_weight, mlp_gate_weight, down_weight = weights
    length = block_piece.shape[0]
    heads_here = decay_rates.shape[0]
    decay_mask, arriving_fading_factor, outgoing_decay = decay_tables(decay_rates, length)
    inputs = block_piece.astype(jnp.float32)
    first_out, first_normed, first_inverse = layer_norm(inputs, first_scale, first_shift)
    first_act = first_out.astype(jnp.bfloat16)
    queries = jnp.dot(first_act, query_weight, preferred_element_type=jnp.float32).astype(jnp.bfloat16)
    key_rows = jnp.dot(first_act, key_weight, preferred_element_type=jnp.float32).astype(jnp.bfloat16)
    value_rows = jnp.dot(first_act, value_weight, preferred_element_type=jnp.float32).astype(jnp.bfloat16)
    gate_pre = jnp.dot(first_act, gate_weight, preferred_element_type=jnp.float32)
    probe_broadcast = queries.reshape(length, heads_here, KD).astype(jnp.float32)
    key_expanded = key_rows.reshape(length, heads_here, KD).astype(jnp.float32)
    value_expanded = value_rows.reshape(length, heads_here, VD).astype(jnp.float32)
    scores = jnp.einsum('ihk,jhk->hij', probe_broadcast, key_expanded) * decay_mask
    retain_weights = scores.astype(jnp.bfloat16)
    retention_expanded = retain_weights.astype(jnp.float32)
    intra_segment_term = jnp.einsum('hij,jhv->ihv', retention_expanded, value_expanded)
    block_local_state = jnp.einsum('xue,xuz->uez', key_expanded * outgoing_decay, value_expanded, precision=FULL_ACCURACY)
    memory_mixer_result = intra_segment_term + arriving_fading_factor * jnp.einsum('qtj,tjz->qtz', probe_broadcast, arriving_memory_matrix, precision=FULL_ACCURACY)
    group_centred = memory_mixer_result - lax.optimization_barrier(jnp.mean(memory_mixer_result, axis=-1, keepdims=True))
    cluster_reciprocal_spread = lax.rsqrt(lax.optimization_barrier(jnp.mean(group_centred * group_centred, axis=-1, keepdims=True)) + EPSILON)
    group_normed = group_centred * cluster_reciprocal_spread
    sigmoid_gate = jax.nn.sigmoid(gate_pre)
    swish_gate = gate_pre * sigmoid_gate
    group_flat = group_normed.reshape(length, heads_here * VD)
    gated_rows = (swish_gate * group_flat).astype(jnp.bfloat16)
    mixer_out = jnp.dot(gated_rows, output_weight, preferred_element_type=jnp.float32)
    hidden_state = inputs + mixer_out
    second_out, second_normed, second_inverse = layer_norm(hidden_state, second_scale, second_shift)
    second_act = second_out.astype(jnp.bfloat16)
    up_pre = jnp.dot(second_act, up_weight, preferred_element_type=jnp.float32)
    mlp_pre = jnp.dot(second_act, mlp_gate_weight, preferred_element_type=jnp.float32)
    gelu_value, gelu_slope = gelu_pair(mlp_pre)
    product = (gelu_value * up_pre).astype(jnp.bfloat16)
    mlp_out = jnp.dot(product, down_weight, preferred_element_type=jnp.float32)
    block_output = (hidden_state + mlp_out).astype(jnp.bfloat16)
    cotangent = cot_piece.astype(jnp.float32)
    down_grad = contract_rows(product, cot_piece)
    product_grad = times_transpose(cot_piece, down_weight)
    up_pre_grad = (product_grad * gelu_value).astype(jnp.bfloat16)
    mlp_pre_grad = (product_grad * up_pre * gelu_slope).astype(jnp.bfloat16)
    up_grad = contract_rows(second_act, up_pre_grad)
    mlp_gate_grad = contract_rows(second_act, mlp_pre_grad)
    second_act_grad = times_transpose(up_pre_grad, up_weight) + times_transpose(mlp_pre_grad, mlp_gate_weight)
    second_scale_grad = lax.optimization_barrier(jnp.sum(second_act_grad * second_normed, axis=0))
    second_shift_grad = lax.optimization_barrier(jnp.sum(second_act_grad, axis=0))
    hidden_grad = cotangent + norm_back(second_act_grad * second_scale, second_normed, second_inverse)
    hidden_cast = hidden_grad.astype(jnp.bfloat16)
    output_grad = contract_rows(gated_rows, hidden_cast)
    gated_grad = times_transpose(hidden_cast, output_weight)
    gate_pre_grad = (gated_grad * group_flat * sigmoid_gate * (1.0 + gate_pre * (1.0 - sigmoid_gate))).astype(jnp.bfloat16)
    normed_grad = (gated_grad * swish_gate).reshape(length, heads_here, VD)
    retained_grad = norm_back(normed_grad, group_normed, cluster_reciprocal_spread).astype(jnp.bfloat16)
    memory_mixer_result_broadcast = retained_grad.astype(jnp.float32)
    state_contribution = jnp.einsum('gdt,gdc->dtc', probe_broadcast * arriving_fading_factor, memory_mixer_result_broadcast, precision=FULL_ACCURACY)
    score_grad = (jnp.einsum('ihv,jhv->hij', memory_mixer_result_broadcast, value_expanded) * decay_mask).astype(jnp.bfloat16)
    scores_expanded = score_grad.astype(jnp.float32)
    query_heads_gradient = (jnp.einsum('uwa,auc->wuc', scores_expanded, key_expanded) + arriving_fading_factor * jnp.einsum('xzu,zwu->xzw', memory_mixer_result_broadcast, arriving_memory_matrix, precision=FULL_ACCURACY)).astype(jnp.bfloat16)
    key_heads_gradient = (jnp.einsum('eus,ueg->seg', scores_expanded, probe_broadcast) + outgoing_decay * jnp.einsum('xwm,wlm->xwl', value_expanded, state_gradient, precision=FULL_ACCURACY)).astype(jnp.bfloat16)
    value_heads_gradient = (jnp.einsum('npl,pnw->lnw', retention_expanded, memory_mixer_result_broadcast) + outgoing_decay * jnp.einsum('wra,rag->wrg', key_expanded, state_gradient, precision=FULL_ACCURACY)).astype(jnp.bfloat16)
    query_flat = query_heads_gradient.reshape(length, heads_here * KD)
    key_flat = key_heads_gradient.reshape(length, heads_here * KD)
    value_flat = value_heads_gradient.reshape(length, heads_here * VD)
    query_grad = contract_rows(first_act, query_flat)
    key_grad = contract_rows(first_act, key_flat)
    value_grad = contract_rows(first_act, value_flat)
    gate_grad = contract_rows(first_act, gate_pre_grad)
    first_act_grad = times_transpose(query_flat, query_weight) + times_transpose(key_flat, key_weight) + times_transpose(value_flat, value_weight) + times_transpose(gate_pre_grad, gate_weight)
    first_scale_grad = lax.optimization_barrier(jnp.sum(first_act_grad * first_normed, axis=0))
    first_shift_grad = lax.optimization_barrier(jnp.sum(first_act_grad, axis=0))
    input_grad = (hidden_grad + norm_back(first_act_grad * first_scale, first_normed, first_inverse)).astype(jnp.bfloat16)
    grad_terms = (first_scale_grad, first_shift_grad, query_grad, key_grad, value_grad, gate_grad, output_grad, second_scale_grad, second_shift_grad, up_grad, mlp_gate_grad, down_grad)
    return (block_output, block_local_state, state_contribution, input_grad, grad_terms)

def reference(block_input, out_cotangent, decay_rate, first_scale, first_shift, query_weight, key_weight, value_weight, gate_weight, output_weight, second_scale, second_shift, up_weight, mlp_gate_weight, down_weight):
    weights = (first_scale, first_shift, query_weight, key_weight, value_weight, gate_weight, output_weight, second_scale, second_shift, up_weight, mlp_gate_weight, down_weight)
    block_count = LENGTH // TOK_DEV
    input_blocks = block_input.reshape(block_count, TOK_DEV, D)
    cot_blocks = out_cotangent.reshape(block_count, TOK_DEV, D)
    block_decay = jnp.exp(-decay_rate * TOK_DEV)[:, None, None]
    empty_state = jnp.zeros((HEADS, KD, VD), jnp.float32)

    def forward_step(state_now, pieces):
        results = layer_block(pieces[0], pieces[1], state_now, empty_state, weights, decay_rate)
        return (block_decay * state_now + results[1], (state_now, results[0], results[2]))
    unused_state, (states_in, output_blocks, state_terms) = lax.scan(forward_step, empty_state, (input_blocks, cot_blocks))

    def suffix_step(carried, state_part):
        return (state_part + block_decay * carried, carried)
    unused_grad, state_grads = lax.scan(suffix_step, empty_state, state_terms, reverse=True)
    zero_grads = tuple((jnp.zeros(weight_item.shape, jnp.float32) for weight_item in weights))

    def backward_step(totals, pieces):
        results = layer_block(pieces[0], pieces[1], pieces[2], pieces[3], weights, decay_rate)
        return (jax.tree.map(jnp.add, totals, results[4]), results[3])
    grad_totals, grad_blocks = lax.scan(backward_step, zero_grads, (input_blocks, cot_blocks, states_in, state_grads))
    return (output_blocks.reshape(LENGTH, D), grad_blocks.reshape(LENGTH, D), grad_totals[0], grad_totals[1], grad_totals[2], grad_totals[3], grad_totals[4], grad_totals[5], grad_totals[6], grad_totals[7], grad_totals[8], grad_totals[9], grad_totals[10], grad_totals[11])
```

```python
import jax
import jax.numpy as jnp
from jax import lax
from jax.sharding import Mesh
from jax.sharding import PartitionSpec as P


KD = 256
VD = 512
SEQ = ("outer", "pair")

EPSILON = 1e-05
F32 = jnp.float32
BF16 = jnp.bfloat16
FULL_ACCURACY = lax.Precision.HIGHEST


def after(x, *events):
    return lax.optimization_barrier((x, *events))[0]


def widen(x):
    return lax.reduce_precision(x.astype(F32), 8, 7)


def narrow(x, zero):
    return (x + zero).astype(BF16)


def flip(x, axis, bit):
    count = lax.axis_size(axis)
    return lax.ppermute(x, axis, [(i, i ^ bit) for i in range(count)])


def bits_of(count):
    bits = []
    while (1 << len(bits)) < count:
        bits.append(1 << len(bits))
    assert (1 << len(bits)) == count
    return bits


def relative_order(count):
    order = [0]
    for bit in reversed(bits_of(count)):
        order = order + [j | bit for j in order]
    return order


def to_relative(x, axis_name, dim):
    count, own = lax.axis_size(axis_name), lax.axis_index(axis_name)
    size = x.shape[dim] // count
    return jnp.concatenate(
        [lax.dynamic_slice_in_dim(x, (own ^ j) * size, size, dim) for j in relative_order(count)],
        axis=dim,
    )


def from_relative(x, axis_name, dim):
    count, own = lax.axis_size(axis_name), lax.axis_index(axis_name)
    size = x.shape[dim] // count
    bits = bits_of(count)
    parts = []
    for i in range(count):
        j = own ^ i
        place = 0
        for n in range(len(bits)):
            place = place + ((j >> n) & 1) * (count >> (n + 1))
        parts.append(lax.dynamic_slice_in_dim(x, place * size, size, dim))
    return jnp.concatenate(parts, axis=dim)


def scatter_rows(x, axis_name):
    for bit in bits_of(lax.axis_size(axis_name)):
        half = x.shape[0] // 2
        x = x[:half] + flip(x[half:], axis_name, bit)
    return x


def gather_rows(x, axis_name):
    for bit in reversed(bits_of(lax.axis_size(axis_name))):
        x = jnp.concatenate([x, flip(x, axis_name, bit)], axis=0)
    return x


def layer_norm(values, scales, shifts):
    centred = values - jnp.mean(values, axis=-1, keepdims=True)
    inverse = lax.rsqrt(jnp.mean(centred * centred, axis=-1, keepdims=True) + EPSILON)
    normed = centred * inverse
    return (normed * scales + shifts, normed, inverse)


def norm_back(upstream, normed, inverse):
    return inverse * (
        upstream
        - jnp.mean(upstream, axis=-1, keepdims=True)
        - normed * jnp.mean(upstream * normed, axis=-1, keepdims=True)
    )


def gelu_pair(pre_act):
    normal_cdf = 0.5 * (1.0 + lax.erf(pre_act * 0.7071067811865476))
    density = jnp.exp(-0.5 * pre_act * pre_act) * 0.3989422804014327
    return (pre_act * normal_cdf, normal_cdf + pre_act * density)


def dot(a, b):
    return jnp.dot(a, b, preferred_element_type=F32)


def contract_rows(left_side, right_side, precision=None):
    return lax.dot_general(
        left_side,
        right_side,
        (((0,), (0,)), ((), ())),
        precision=precision,
        preferred_element_type=F32,
    )


def times_transpose(left_side, right_side, precision=None):
    return lax.dot_general(
        left_side,
        right_side,
        (((1,), (1,)), ((), ())),
        precision=precision,
        preferred_element_type=F32,
    )


def from_partner(x, zero):
    return narrow(flip(widen(x), "pair", 1), zero)


def carry_states(local, decay, suffix, event=None):
    pairs, odd = lax.axis_size("outer"), lax.axis_index("pair")
    if suffix:
        odd = 1 - odd
    half = local.shape[1] // 2
    keep = lax.dynamic_slice_in_dim(local, odd * half, half, 1)
    give = lax.dynamic_slice_in_dim(local, (1 - odd) * half, half, 1)
    got = flip(give, "pair", 1)
    if event is not None:
        got = after(got, event)
    earlier = jnp.where(odd == 0, keep, got)
    later = jnp.where(odd == 0, got, keep)
    step = decay[:, None, None]
    total = step * earlier + later

    def shifted(x, distance, first):
        moves = [(i, i + distance) for i in range(first, pairs - distance)]
        if suffix:
            moves = [(pairs - 1 - i, pairs - 1 - j) for i, j in moves]
        return lax.ppermute(x, "outer", moves)

    arriving = shifted(total, 1, 0)
    factor = step * step
    distance = 1
    while distance < pairs - 1:
        arriving = arriving + factor * shifted(arriving, distance, 1)
        factor = factor * factor
        distance *= 2
    second = step * arriving + earlier
    mine = jnp.where(odd == 0, arriving, second)
    other = jnp.where(odd == 0, second, arriving)
    rest = flip(other, "pair", 1)
    return jnp.where(
        odd == 0,
        jnp.concatenate([mine, rest], axis=1),
        jnp.concatenate([rest, mine], axis=1),
    )


def split_columns(x):
    outer, place = lax.axis_size("outer"), lax.axis_index("pair")
    size = x.shape[1] // (2 * outer)

    def blocks(which):
        return jnp.concatenate(
            [lax.dynamic_slice_in_dim(x, (2 * o + which) * size, size, 1) for o in range(outer)],
            axis=1,
        )

    return blocks(place), blocks(1 - place)


def sum_blocks(x, dim):
    return lax.psum_scatter(x, "outer", scatter_dimension=dim, tiled=True)


def shards(
    block_input,
    out_cotangent,
    decay_rate,
    first_scale,
    first_shift,
    query_weight,
    key_weight,
    value_weight,
    gate_weight,
    output_weight,
    second_scale,
    second_shift,
    up_weight,
    mlp_gate_weight,
    down_weight,
):
    length, _ = block_input.shape
    local_heads = decay_rate.shape[0]
    head_range = range(local_heads)
    zero = decay_rate[0] * 0.0

    places = jnp.arange(length, dtype=F32)
    distance = places[:, None] - places[None, :]
    causal = distance >= 0.0
    safe = jnp.where(causal, distance, 0.0)
    masks = [jnp.where(causal, jnp.exp(-decay_rate[h] * safe), 0.0) for h in head_range]
    fade_in = [jnp.exp(-places * decay_rate[h])[:, None] for h in head_range]
    fade_out = [jnp.exp(-(length - places) * decay_rate[h])[:, None] for h in head_range]
    block_decay = jnp.exp(-decay_rate * length)

    inputs = block_input.astype(F32)
    first_out, first_normed, first_inverse = layer_norm(inputs, first_scale, first_shift)
    first_act = first_out.astype(BF16)
    queries = dot(first_act, query_weight).astype(BF16)
    key_rows = dot(first_act, key_weight).astype(BF16)
    value_rows = dot(first_act, value_weight).astype(BF16)
    q = [queries[:, h * KD : (h + 1) * KD] for h in head_range]
    k = [key_rows[:, h * KD : (h + 1) * KD] for h in head_range]
    v = [value_rows[:, h * VD : (h + 1) * VD] for h in head_range]
    local_state = jnp.stack(
        [
            contract_rows(k[h].astype(F32) * fade_out[h], v[h].astype(F32), FULL_ACCURACY)
            for h in head_range
        ]
    )
    state_in = carry_states(local_state, block_decay, False)

    gate_pre = dot(first_act, gate_weight)
    sigmoid_gate = jax.nn.sigmoid(gate_pre)
    swish_gate = gate_pre * sigmoid_gate
    retain_weights = [(times_transpose(q[h], k[h]) * masks[h]).astype(BF16) for h in head_range]
    group_normed, spread = [], []
    for h in head_range:
        retained = dot(retain_weights[h], v[h]) + fade_in[h] * jnp.dot(
            q[h].astype(F32), state_in[h], precision=FULL_ACCURACY
        )
        centred = retained - jnp.mean(retained, axis=-1, keepdims=True)
        inverse = lax.rsqrt(jnp.mean(centred * centred, axis=-1, keepdims=True) + EPSILON)
        group_normed.append(centred * inverse)
        spread.append(inverse)
    gated_rows = jnp.concatenate(
        [swish_gate[:, h * VD : (h + 1) * VD] * group_normed[h] for h in head_range], axis=1
    ).astype(BF16)
    gated_rel = to_relative(gated_rows, "head", 0)
    own_rows = length // lax.axis_size("head")
    row_start = lax.axis_index("head") * own_rows
    input_rows = lax.dynamic_slice_in_dim(inputs, row_start, own_rows, 0)
    cot_rows = lax.dynamic_slice_in_dim(out_cotangent, row_start, own_rows, 0).astype(F32)

    cot_rel = to_relative(out_cotangent, "head", 0)
    cot_kept, cot_given = split_columns(cot_rel)
    cot_pair = jnp.concatenate([cot_kept, from_partner(after(cot_given, state_in), zero)])

    hidden = input_rows + scatter_rows(dot(gated_rel, output_weight), "head")
    second_out, second_normed, second_inverse = layer_norm(hidden, second_scale, second_shift)
    second_rows = widen(second_out)
    second_act = narrow(gather_rows(second_rows, "head"), zero)
    second_given = flip(split_columns(second_rows)[1], "pair", 1)

    first_kept, first_given = split_columns(first_act)
    first_given = flip(after(widen(first_given), second_rows), "pair", 1)

    up_pre = dot(second_act, up_weight)
    mlp_pre = dot(second_act, mlp_gate_weight)
    gelu_value, gelu_slope = gelu_pair(mlp_pre)
    product = (gelu_value * up_pre).astype(BF16)
    product_given = flip(widen(product), "pair", 1)

    product_grad = times_transpose(cot_rel, down_weight)
    up_pre_grad = (product_grad * gelu_value).astype(BF16)
    mlp_pre_grad = (product_grad * up_pre * gelu_slope).astype(BF16)
    mlp_grads = jnp.concatenate([up_pre_grad, mlp_pre_grad], axis=1)
    mlp_given = flip(widen(mlp_grads), "pair", 1)
    second_act_grad = scatter_rows(
        times_transpose(up_pre_grad, up_weight) + times_transpose(mlp_pre_grad, mlp_gate_weight),
        "head",
    )
    hidden_grad = cot_rows + norm_back(
        second_act_grad * second_scale, second_normed, second_inverse
    )
    cast_rows = widen(hidden_grad)
    cast_all = gather_rows(cast_rows, "head")

    product_pair = jnp.concatenate([product, narrow(after(product_given, cast_rows), zero)])
    down_term = contract_rows(cot_pair, product_pair)
    down_grad = sum_blocks(down_term, 0).T

    hidden_cast = from_relative(narrow(after(cast_all, down_term), zero), "head", 0)
    gated_grad = times_transpose(hidden_cast, output_weight)
    group_flat = jnp.concatenate(group_normed, axis=1)
    gate_pre_grad = (
        gated_grad * group_flat * sigmoid_gate * (1.0 + gate_pre * (1.0 - sigmoid_gate))
    ).astype(BF16)
    normed_grad = gated_grad * swish_gate
    retained_grad = [
        norm_back(normed_grad[:, h * VD : (h + 1) * VD], group_normed[h], spread[h]).astype(BF16)
        for h in head_range
    ]
    state_term = jnp.stack(
        [
            contract_rows(
                q[h].astype(F32) * fade_in[h], retained_grad[h].astype(F32), FULL_ACCURACY
            )
            for h in head_range
        ]
    )
    cast_given = flip(split_columns(cast_rows)[1], "pair", 1)
    gated_given = flip(after(widen(gated_rows), cast_rows), "pair", 1)
    gate_given = flip(widen(gate_pre_grad), "pair", 1)

    second_given = narrow(gather_rows(second_given, "head"), zero)
    second_pair = jnp.concatenate([split_columns(second_act)[0], second_given])
    mlp_pair = jnp.concatenate([mlp_grads, narrow(after(mlp_given, state_term), zero)])
    mlp_term = contract_rows(second_pair, mlp_pair)
    up_both = sum_blocks(mlp_term, 0)
    state_grad = carry_states(state_term, block_decay, True, mlp_term)
    hidden_units = up_weight.shape[1]
    up_grad, mlp_gate_grad = up_both[:, :hidden_units], up_both[:, hidden_units:]

    output_rows = hidden + scatter_rows(dot(product, after(down_weight, cast_rows)), "head")
    output_rows = widen(output_rows)
    block_output = from_relative(narrow(gather_rows(output_rows, "head"), zero), "head", 0)

    second_scale_part = jnp.sum(second_act_grad * second_normed, axis=0)
    second_shift_part = jnp.sum(second_act_grad, axis=0)

    query_parts, key_parts, value_parts = [], [], []
    for h in head_range:
        score_grad = (times_transpose(retained_grad[h], v[h]) * masks[h]).astype(BF16)
        query_parts.append(
            dot(score_grad, k[h])
            + fade_in[h]
            * times_transpose(retained_grad[h].astype(F32), state_in[h], FULL_ACCURACY)
        )
        key_parts.append(
            contract_rows(score_grad, q[h])
            + fade_out[h] * times_transpose(v[h].astype(F32), state_grad[h], FULL_ACCURACY)
        )
        value_parts.append(
            contract_rows(retain_weights[h], retained_grad[h])
            + fade_out[h]
            * jnp.dot(k[h].astype(F32), state_grad[h], precision=FULL_ACCURACY)
        )
    head_grads = jnp.concatenate(query_parts + key_parts + value_parts, axis=1).astype(BF16)
    head_given = flip(widen(head_grads), "pair", 1)

    cast_given = from_relative(narrow(gather_rows(cast_given, "head"), zero), "head", 0)
    cast_pair = jnp.concatenate([split_columns(hidden_cast)[0], cast_given])
    gated_pair = jnp.concatenate([gated_rows, narrow(gated_given, zero)])
    first_pair = jnp.concatenate([first_kept, narrow(after(first_given, head_grads), zero)])
    gate_pair = jnp.concatenate([gate_pre_grad, narrow(gate_given, zero)])
    output_term = jnp.concatenate(
        [contract_rows(cast_pair, gated_pair), contract_rows(first_pair, gate_pair)], axis=1
    )
    output_both = sum_blocks(output_term, 0)
    output_columns = gated_rows.shape[1]
    output_grad, gate_grad = output_both[:, :output_columns].T, output_both[:, output_columns:]

    head_pair = jnp.concatenate([head_grads, narrow(after(head_given, output_term), zero)])
    head_both = sum_blocks(contract_rows(first_pair, head_pair), 0)
    key_columns, value_columns = local_heads * KD, 2 * local_heads * KD
    query_grad = head_both[:, :key_columns]
    key_grad = head_both[:, key_columns:value_columns]
    value_grad = head_both[:, value_columns:]

    first_act_grad = (
        times_transpose(head_grads[:, :key_columns], query_weight)
        + times_transpose(head_grads[:, key_columns:value_columns], key_weight)
        + times_transpose(head_grads[:, value_columns:], value_weight)
        + times_transpose(gate_pre_grad, gate_weight)
    )
    first_act_grad = scatter_rows(to_relative(first_act_grad, "head", 0), "head")
    normed_rows = lax.dynamic_slice_in_dim(first_normed, row_start, own_rows, 0)
    inverse_rows = lax.dynamic_slice_in_dim(first_inverse, row_start, own_rows, 0)
    first_scale_part = jnp.sum(first_act_grad * normed_rows, axis=0)
    first_shift_part = jnp.sum(first_act_grad, axis=0)
    grad_rows = hidden_grad + norm_back(first_act_grad * first_scale, normed_rows, inverse_rows)
    grad_rows = widen(grad_rows)
    input_grad = from_relative(narrow(gather_rows(grad_rows, "head"), zero), "head", 0)

    vectors = jnp.stack([first_scale_part, first_shift_part, second_scale_part, second_shift_part])
    kept, given = split_columns(vectors)
    vectors = kept + flip(given, "pair", 1)
    vectors = to_relative(vectors, "outer", 1)
    for bit in bits_of(lax.axis_size("outer")):
        half = vectors.shape[1] // 2
        vectors = vectors[:, :half] + flip(vectors[:, half:], "outer", bit)
    for bit in bits_of(lax.axis_size("head")):
        vectors = vectors + flip(vectors, "head", bit)
    return (
        block_output,
        input_grad,
        vectors[0],
        vectors[1],
        query_grad,
        key_grad,
        value_grad,
        gate_grad,
        output_grad,
        vectors[2],
        vectors[3],
        up_grad,
        mlp_gate_grad,
        down_grad,
    )


def solution(mesh):
    seq, head = mesh.shape["seq"], mesh.shape["head"]
    mesh = Mesh(mesh.devices.reshape(seq // 2, 2, head), ("outer", "pair", "head"))
    in_specs = (
        P(SEQ, None),
        P(SEQ, None),
        P("head"),
        P(),
        P(),
        P(None, "head"),
        P(None, "head"),
        P(None, "head"),
        P(None, "head"),
        P("head", None),
        P(),
        P(),
        P(None, "head"),
        P(None, "head"),
        P("head", None),
    )
    out_specs = (
        P(SEQ, None),
        P(SEQ, None),
        P(SEQ),
        P(SEQ),
        P(SEQ, "head"),
        P(SEQ, "head"),
        P(SEQ, "head"),
        P(SEQ, "head"),
        P("head", SEQ),
        P(SEQ),
        P(SEQ),
        P(SEQ, "head"),
        P(SEQ, "head"),
        P("head", SEQ),
    )

    def step(*args):
        return shards(*args)

    step = jax.shard_map(step, mesh=mesh, in_specs=in_specs, out_specs=out_specs, check_vma=False)
    return step
```

```python
import functools

import jax
import jax.numpy as jnp
from jax import lax
from jax.experimental import pallas as pl
from jax.experimental.pallas import tpu as pltpu
from jax.sharding import Mesh
from jax.sharding import PartitionSpec as P


KD = 256
VD = 512
SEQ = ("outer", "pair")

EPSILON = 1e-05
F32 = jnp.float32
BF16 = jnp.bfloat16
FULL_ACCURACY = lax.Precision.HIGHEST


def after(x, *events):
    return lax.optimization_barrier((x, *events))[0]


def widen(x):
    return lax.reduce_precision(x.astype(F32), 8, 7)


def narrow(x, zero):
    return (x + zero).astype(BF16)


def flip(x, axis, bit):
    count = lax.axis_size(axis)
    return lax.ppermute(x, axis, [(i, i ^ bit) for i in range(count)])


def bits_of(count):
    bits = []
    while (1 << len(bits)) < count:
        bits.append(1 << len(bits))
    assert (1 << len(bits)) == count
    return bits


def relative_order(count):
    order = [0]
    for bit in reversed(bits_of(count)):
        order = order + [j | bit for j in order]
    return order


def to_relative(x, axis_name, dim):
    count, own = lax.axis_size(axis_name), lax.axis_index(axis_name)
    size = x.shape[dim] // count
    return jnp.concatenate(
        [lax.dynamic_slice_in_dim(x, (own ^ j) * size, size, dim) for j in relative_order(count)],
        axis=dim,
    )


def from_relative(x, axis_name, dim):
    count, own = lax.axis_size(axis_name), lax.axis_index(axis_name)
    size = x.shape[dim] // count
    bits = bits_of(count)
    parts = []
    for i in range(count):
        j = own ^ i
        place = 0
        for n in range(len(bits)):
            place = place + ((j >> n) & 1) * (count >> (n + 1))
        parts.append(lax.dynamic_slice_in_dim(x, place * size, size, dim))
    return jnp.concatenate(parts, axis=dim)


def scatter_rows(x, axis_name):
    for bit in bits_of(lax.axis_size(axis_name)):
        half = x.shape[0] // 2
        x = x[:half] + flip(x[half:], axis_name, bit)
    return x


def gather_rows(x, axis_name):
    for bit in reversed(bits_of(lax.axis_size(axis_name))):
        x = jnp.concatenate([x, flip(x, axis_name, bit)], axis=0)
    return x


def layer_norm(values, scales, shifts):
    centred = values - jnp.mean(values, axis=-1, keepdims=True)
    inverse = lax.rsqrt(jnp.mean(centred * centred, axis=-1, keepdims=True) + EPSILON)
    normed = centred * inverse
    return (normed * scales + shifts, normed, inverse)


def norm_back(upstream, normed, inverse):
    return inverse * (
        upstream
        - jnp.mean(upstream, axis=-1, keepdims=True)
        - normed * jnp.mean(upstream * normed, axis=-1, keepdims=True)
    )


def gelu_pair(pre_act):
    normal_cdf = 0.5 * (1.0 + lax.erf(pre_act * 0.7071067811865476))
    density = jnp.exp(-0.5 * pre_act * pre_act) * 0.3989422804014327
    return (pre_act * normal_cdf, normal_cdf + pre_act * density)


def dot(a, b):
    return jnp.dot(a, b, preferred_element_type=F32)


def contract_rows(left_side, right_side, precision=None):
    return lax.dot_general(
        left_side,
        right_side,
        (((0,), (0,)), ((), ())),
        precision=precision,
        preferred_element_type=F32,
    )


def times_transpose(left_side, right_side, precision=None):
    return lax.dot_general(
        left_side,
        right_side,
        (((1,), (1,)), ((), ())),
        precision=precision,
        preferred_element_type=F32,
    )


def from_partner(x, zero):
    return narrow(flip(widen(x), "pair", 1), zero)


def carry_states(local, decay, suffix, event=None):
    pairs, odd = lax.axis_size("outer"), lax.axis_index("pair")
    if suffix:
        odd = 1 - odd
    half = local.shape[1] // 2
    keep = lax.dynamic_slice_in_dim(local, odd * half, half, 1)
    give = lax.dynamic_slice_in_dim(local, (1 - odd) * half, half, 1)
    got = flip(give, "pair", 1)
    if event is not None:
        got = after(got, event)
    earlier = jnp.where(odd == 0, keep, got)
    later = jnp.where(odd == 0, got, keep)
    step = decay[:, None, None]
    total = step * earlier + later

    arriving = jnp.zeros_like(total)
    for hop in range(pairs - 1):
        way = (pairs - 1 - hop, pairs - 2 - hop) if suffix else (hop, hop + 1)
        leaving = step * step * arriving + total if hop else total
        arriving = arriving + lax.ppermute(leaving, "outer", [way])
    second = step * arriving + earlier
    mine = jnp.where(odd == 0, arriving, second)
    other = jnp.where(odd == 0, second, arriving)
    rest = flip(other, "pair", 1)
    return jnp.where(
        odd == 0,
        jnp.concatenate([mine, rest], axis=1),
        jnp.concatenate([rest, mine], axis=1),
    )


def scan_kernel(
    pairs,
    pieces,
    decay_ref,
    rate_ref,
    local_ref,
    act_ref,
    gate_weight_ref,
    query_ref,
    key_ref,
    value_ref,
    state_ref,
    gate_ref,
    weights_ref,
    intra_ref,
    got,
    arriving,
    leaving,
    other,
    rest,
    give_send,
    give_recv,
    chain_send,
    chain_recv,
    rest_send,
    rest_recv,
):
    heads, rows, _ = local_ref.shape
    half = rows // 2
    count = heads * pieces
    size = half // pieces
    outer, odd = lax.axis_index("outer"), lax.axis_index("pair")
    is_odd = odd == 1
    has_earlier, has_later = outer > 0, outer < pairs - 1
    partner = {"pair": 1 - odd}

    barrier = pltpu.get_barrier_semaphore()
    pl.semaphore_signal(barrier, device_id=partner, device_id_type=pl.DeviceIdType.MESH)

    @pl.when(has_earlier)
    def _():
        pl.semaphore_signal(
            barrier, device_id={"outer": outer - 1}, device_id_type=pl.DeviceIdType.MESH
        )

    pl.semaphore_wait(barrier, jnp.where(has_later, 2, 1))

    def rows_of(i, which):
        start = which * half + (i % pieces) * size
        return i // pieces, pl.ds(pl.multiple_of(start, size), size)

    def give(i):
        head, place = rows_of(i, 1 - odd)
        return pltpu.make_async_remote_copy(
            src_ref=local_ref.at[head, place],
            dst_ref=got.at[i],
            send_sem=give_send.at[i],
            recv_sem=give_recv.at[i],
            device_id=partner,
            device_id_type=pl.DeviceIdType.MESH,
        )

    def onward(i):
        return pltpu.make_async_remote_copy(
            src_ref=leaving.at[i],
            dst_ref=arriving.at[i],
            send_sem=chain_send.at[i],
            recv_sem=chain_recv.at[i],
            device_id={"outer": outer + 1},
            device_id_type=pl.DeviceIdType.MESH,
        )

    def finish(i):
        return pltpu.make_async_remote_copy(
            src_ref=other.at[i],
            dst_ref=rest.at[i],
            send_sem=rest_send.at[i],
            recv_sem=rest_recv.at[i],
            device_id=partner,
            device_id_type=pl.DeviceIdType.MESH,
        )

    for i in range(count):
        give(i).start()

    columns = gate_weight_ref.shape[1]
    tile = columns // 4

    def gate_tile(n):
        place = pl.ds(n * tile, tile)
        gate_ref[:, place] = jnp.dot(
            act_ref[...], gate_weight_ref[:, place], preferred_element_type=F32
        )

    def scores(h):
        q = query_ref[:, h * KD : (h + 1) * KD]
        k = key_ref[:, h * KD : (h + 1) * KD]
        length = q.shape[0]
        value = times_transpose(q, k)
        place = lax.broadcasted_iota(jnp.int32, (length, length), 0)
        place = place - lax.broadcasted_iota(jnp.int32, (length, length), 1)
        fading = jnp.exp(-rate_ref[h] * jnp.maximum(place, 0).astype(F32))
        weights_ref[h] = jnp.where(place >= 0, value * fading, 0.0).astype(BF16)

    def intra(h):
        intra_ref[h] = jnp.dot(
            weights_ref[h], value_ref[:, h * VD : (h + 1) * VD], preferred_element_type=F32
        )

    work = [functools.partial(gate_tile, n) for n in range(4)]
    for h in range(heads):
        work.append(functools.partial(scores, h))
        work.append(functools.partial(intra, h))
    per_piece = -(-(len(work) - 2) // count)
    for job in work[:2]:
        job()
    work = work[2:]

    for i in range(count):
        head, kept_rows = rows_of(i, odd)
        give(i).wait_recv()
        kept, came = local_ref[head, kept_rows], got[i]
        earlier = jnp.where(is_odd, came, kept)
        later = jnp.where(is_odd, kept, came)
        decay = decay_ref[head]

        @pl.when(has_earlier)
        def _():
            onward(i).wait_recv()

        @pl.when(jnp.logical_not(has_earlier))
        def _():
            arriving[i] = jnp.zeros_like(came)

        state = arriving[i]
        second = decay * state + earlier

        @pl.when(has_later)
        def _():
            leaving[i] = decay * second + later
            onward(i).start()

        other[i] = jnp.where(is_odd, state, second)
        finish(i).start()
        state_ref[head, kept_rows] = jnp.where(is_odd, second, state)
        for job in work[:per_piece]:
            job()
        work = work[per_piece:]
    for i in range(count):
        head, place = rows_of(i, 1 - odd)
        finish(i).wait_recv()
        state_ref[head, place] = rest[i]
    for i in range(count):
        give(i).wait_send()
        finish(i).wait_send()

        @pl.when(has_later)
        def _():
            onward(i).wait_send()


def scan_states(local, decay, rate, act, gate_weight, queries, key_rows, value_rows):
    heads, rows, columns = local.shape
    length = act.shape[0]
    pieces = 2
    count = heads * pieces
    buffer = pltpu.VMEM((count, rows // 2 // pieces, columns), F32)
    vector = pl.BlockSpec(memory_space=pltpu.VMEM)
    scalar = pl.BlockSpec(memory_space=pltpu.SMEM)
    return pl.pallas_call(
        functools.partial(scan_kernel, lax.axis_size("outer"), pieces),
        out_shape=(
            jax.ShapeDtypeStruct(local.shape, F32),
            jax.ShapeDtypeStruct((length, gate_weight.shape[1]), F32),
            jax.ShapeDtypeStruct((heads, length, length), BF16),
            jax.ShapeDtypeStruct((heads, length, VD), F32),
        ),
        in_specs=[scalar, scalar] + [vector] * 6,
        out_specs=(vector,) * 4,
        scratch_shapes=[buffer] * 5 + [pltpu.SemaphoreType.DMA((count,))] * 6,
        compiler_params=pltpu.CompilerParams(
            collective_id=0, has_side_effects=True, vmem_limit_bytes=40 * 1024 * 1024
        ),
        cost_estimate=pl.CostEstimate(
            flops=2 * length * act.shape[1] * gate_weight.shape[1],
            bytes_accessed=16 * 1024 * 1024,
            transcendentals=heads * length * length,
        ),
    )(decay, rate, local, act, gate_weight, queries, key_rows, value_rows)


def split_columns(x):
    outer, place = lax.axis_size("outer"), lax.axis_index("pair")
    size = x.shape[1] // (2 * outer)

    def blocks(which):
        return jnp.concatenate(
            [lax.dynamic_slice_in_dim(x, (2 * o + which) * size, size, 1) for o in range(outer)],
            axis=1,
        )

    return blocks(place), blocks(1 - place)


def sum_blocks(x):
    return lax.psum_scatter(x, "outer", scatter_dimension=0, tiled=True)


def shards(
    block_input,
    out_cotangent,
    decay_rate,
    first_scale,
    first_shift,
    query_weight,
    key_weight,
    value_weight,
    gate_weight,
    output_weight,
    second_scale,
    second_shift,
    up_weight,
    mlp_gate_weight,
    down_weight,
):
    length, _ = block_input.shape
    local_heads = decay_rate.shape[0]
    head_range = range(local_heads)
    zero = decay_rate[0] * 0.0

    places = jnp.arange(length, dtype=F32)
    distance = places[:, None] - places[None, :]
    causal = distance >= 0.0
    safe = jnp.where(causal, distance, 0.0)
    masks = [jnp.where(causal, jnp.exp(-decay_rate[h] * safe), 0.0) for h in head_range]
    fade_in = [jnp.exp(-places * decay_rate[h])[:, None] for h in head_range]
    fade_out = [jnp.exp(-(length - places) * decay_rate[h])[:, None] for h in head_range]
    block_decay = jnp.exp(-decay_rate * length)

    inputs = block_input.astype(F32)
    first_out, first_normed, first_inverse = layer_norm(inputs, first_scale, first_shift)
    first_act = first_out.astype(BF16)
    queries = dot(first_act, query_weight).astype(BF16)
    key_rows = dot(first_act, key_weight).astype(BF16)
    value_rows = dot(first_act, value_weight).astype(BF16)
    q = [queries[:, h * KD : (h + 1) * KD] for h in head_range]
    k = [key_rows[:, h * KD : (h + 1) * KD] for h in head_range]
    v = [value_rows[:, h * VD : (h + 1) * VD] for h in head_range]
    local_state = jnp.stack(
        [
            contract_rows(k[h].astype(F32) * fade_out[h], v[h].astype(F32), FULL_ACCURACY)
            for h in head_range
        ]
    )
    state_in, gate_pre, retain_weights, intra = scan_states(
        local_state,
        block_decay,
        decay_rate,
        first_act,
        gate_weight,
        queries,
        key_rows,
        value_rows,
    )

    sigmoid_gate = jax.nn.sigmoid(gate_pre)
    swish_gate = gate_pre * sigmoid_gate
    group_normed, spread = [], []
    for h in head_range:
        retained = intra[h] + fade_in[h] * jnp.dot(
            q[h].astype(F32), state_in[h], precision=FULL_ACCURACY
        )
        centred = retained - jnp.mean(retained, axis=-1, keepdims=True)
        inverse = lax.rsqrt(jnp.mean(centred * centred, axis=-1, keepdims=True) + EPSILON)
        group_normed.append(centred * inverse)
        spread.append(inverse)
    gated_rows = jnp.concatenate(
        [swish_gate[:, h * VD : (h + 1) * VD] * group_normed[h] for h in head_range], axis=1
    ).astype(BF16)
    gated_rel = to_relative(gated_rows, "head", 0)
    own_rows = length // lax.axis_size("head")
    row_start = lax.axis_index("head") * own_rows
    input_rows = lax.dynamic_slice_in_dim(inputs, row_start, own_rows, 0)
    cot_rows = lax.dynamic_slice_in_dim(out_cotangent, row_start, own_rows, 0).astype(F32)

    cot_rel = to_relative(out_cotangent, "head", 0)
    cot_kept, cot_given = split_columns(cot_rel)
    cot_pair = jnp.concatenate([cot_kept, from_partner(after(cot_given, state_in), zero)])

    hidden = input_rows + scatter_rows(dot(gated_rel, output_weight), "head")
    second_out, second_normed, second_inverse = layer_norm(hidden, second_scale, second_shift)
    second_rows = widen(second_out)
    second_act = narrow(gather_rows(second_rows, "head"), zero)
    second_given = flip(split_columns(second_rows)[1], "pair", 1)

    first_kept, first_given = split_columns(first_act)
    first_given = flip(after(widen(first_given), second_rows), "pair", 1)

    up_pre = dot(second_act, up_weight)
    mlp_pre = dot(second_act, mlp_gate_weight)
    gelu_value, gelu_slope = gelu_pair(mlp_pre)
    product = (gelu_value * up_pre).astype(BF16)
    product_given = flip(widen(product), "pair", 1)

    product_grad = times_transpose(cot_rel, down_weight)
    up_pre_grad = (product_grad * gelu_value).astype(BF16)
    mlp_pre_grad = (product_grad * up_pre * gelu_slope).astype(BF16)
    mlp_grads = jnp.concatenate([up_pre_grad, mlp_pre_grad], axis=1)
    mlp_given = flip(widen(mlp_grads), "pair", 1)
    second_act_grad = times_transpose(up_pre_grad, up_weight) + times_transpose(
        mlp_pre_grad, mlp_gate_weight
    )
    second_act_grad = scatter_rows(second_act_grad, "head")
    hidden_grad = cot_rows + norm_back(
        second_act_grad * second_scale, second_normed, second_inverse
    )
    cast_rows = widen(hidden_grad)
    cast_all = gather_rows(cast_rows, "head")

    product_pair = jnp.concatenate([product, narrow(after(product_given, cast_rows), zero)])
    down_term = contract_rows(cot_pair, product_pair)
    down_grad = sum_blocks(down_term).T

    hidden_cast = from_relative(narrow(after(cast_all, down_term), zero), "head", 0)
    gated_grad = times_transpose(hidden_cast, output_weight)
    group_flat = jnp.concatenate(group_normed, axis=1)
    gate_pre_grad = (
        gated_grad * group_flat * sigmoid_gate * (1.0 + gate_pre * (1.0 - sigmoid_gate))
    ).astype(BF16)
    normed_grad = gated_grad * swish_gate
    retained_grad = [
        norm_back(normed_grad[:, h * VD : (h + 1) * VD], group_normed[h], spread[h]).astype(BF16)
        for h in head_range
    ]
    state_term = jnp.stack(
        [
            contract_rows(
                q[h].astype(F32) * fade_in[h], retained_grad[h].astype(F32), FULL_ACCURACY
            )
            for h in head_range
        ]
    )
    cast_given = flip(split_columns(cast_rows)[1], "pair", 1)
    gated_given = flip(after(widen(gated_rows), cast_rows), "pair", 1)
    gate_given = flip(widen(gate_pre_grad), "pair", 1)

    second_given = narrow(gather_rows(second_given, "head"), zero)
    second_pair = jnp.concatenate([split_columns(second_act)[0], second_given])
    mlp_pair = jnp.concatenate([mlp_grads, narrow(after(mlp_given, state_term), zero)])
    mlp_term = contract_rows(second_pair, mlp_pair)
    mlp_both = sum_blocks(mlp_term)
    hidden_units = up_weight.shape[1]
    up_grad, mlp_gate_grad = mlp_both[:, :hidden_units], mlp_both[:, hidden_units:]
    state_grad = carry_states(state_term, block_decay, True, mlp_term)

    output_rows = hidden + scatter_rows(dot(product, after(down_weight, cast_rows)), "head")
    output_rows = widen(output_rows)
    block_output = from_relative(narrow(gather_rows(output_rows, "head"), zero), "head", 0)

    second_scale_part = jnp.sum(second_act_grad * second_normed, axis=0)
    second_shift_part = jnp.sum(second_act_grad, axis=0)

    query_parts, key_parts, value_parts = [], [], []
    for h in head_range:
        score_grad = (times_transpose(retained_grad[h], v[h]) * masks[h]).astype(BF16)
        query_parts.append(
            dot(score_grad, k[h])
            + fade_in[h]
            * times_transpose(retained_grad[h].astype(F32), state_in[h], FULL_ACCURACY)
        )
        key_parts.append(
            contract_rows(score_grad, q[h])
            + fade_out[h] * times_transpose(v[h].astype(F32), state_grad[h], FULL_ACCURACY)
        )
        value_parts.append(
            contract_rows(retain_weights[h], retained_grad[h])
            + fade_out[h]
            * jnp.dot(k[h].astype(F32), state_grad[h], precision=FULL_ACCURACY)
        )
    head_grads = jnp.concatenate(query_parts + key_parts + value_parts, axis=1).astype(BF16)
    head_given = flip(widen(head_grads), "pair", 1)

    cast_given = from_relative(narrow(gather_rows(cast_given, "head"), zero), "head", 0)
    cast_pair = jnp.concatenate([split_columns(hidden_cast)[0], cast_given])
    gated_pair = jnp.concatenate([gated_rows, narrow(gated_given, zero)])
    first_pair = jnp.concatenate([first_kept, narrow(first_given, zero)])
    gate_pair = jnp.concatenate([gate_pre_grad, narrow(gate_given, zero)])
    output_term = jnp.concatenate(
        [contract_rows(cast_pair, gated_pair), contract_rows(first_pair, gate_pair)], axis=1
    )
    output_both = sum_blocks(output_term)
    output_columns = gated_rows.shape[1]
    output_grad, gate_grad = output_both[:, :output_columns].T, output_both[:, output_columns:]

    head_pair = jnp.concatenate([head_grads, narrow(after(head_given, output_term), zero)])
    head_both = sum_blocks(contract_rows(first_pair, head_pair))
    key_columns, value_columns = local_heads * KD, 2 * local_heads * KD
    query_grad = head_both[:, :key_columns]
    key_grad = head_both[:, key_columns:value_columns]
    value_grad = head_both[:, value_columns:]

    first_act_grad = (
        times_transpose(head_grads[:, :key_columns], query_weight)
        + times_transpose(head_grads[:, key_columns:value_columns], key_weight)
        + times_transpose(head_grads[:, value_columns:], value_weight)
        + times_transpose(gate_pre_grad, gate_weight)
    )
    first_act_grad = scatter_rows(to_relative(first_act_grad, "head", 0), "head")
    normed_rows = lax.dynamic_slice_in_dim(first_normed, row_start, own_rows, 0)
    inverse_rows = lax.dynamic_slice_in_dim(first_inverse, row_start, own_rows, 0)
    first_scale_part = jnp.sum(first_act_grad * normed_rows, axis=0)
    first_shift_part = jnp.sum(first_act_grad, axis=0)
    grad_rows = hidden_grad + norm_back(first_act_grad * first_scale, normed_rows, inverse_rows)
    grad_rows = widen(grad_rows)
    input_grad = from_relative(narrow(gather_rows(grad_rows, "head"), zero), "head", 0)

    vectors = jnp.stack([first_scale_part, first_shift_part, second_scale_part, second_shift_part])
    kept, given = split_columns(vectors)
    vectors = kept + flip(given, "pair", 1)
    vectors = to_relative(vectors, "outer", 1)
    for bit in bits_of(lax.axis_size("outer")):
        half = vectors.shape[1] // 2
        vectors = vectors[:, :half] + flip(vectors[:, half:], "outer", bit)
    for bit in bits_of(lax.axis_size("head")):
        vectors = vectors + flip(vectors, "head", bit)
    return (
        block_output,
        input_grad,
        vectors[0],
        vectors[1],
        query_grad,
        key_grad,
        value_grad,
        gate_grad,
        output_grad,
        vectors[2],
        vectors[3],
        up_grad,
        mlp_gate_grad,
        down_grad,
    )


def solution(mesh):
    seq, head = mesh.shape["seq"], mesh.shape["head"]
    mesh = Mesh(mesh.devices.reshape(seq // 2, 2, head), ("outer", "pair", "head"))
    in_specs = (
        P(SEQ, None),
        P(SEQ, None),
        P("head"),
        P(),
        P(),
        P(None, "head"),
        P(None, "head"),
        P(None, "head"),
        P(None, "head"),
        P("head", None),
        P(),
        P(),
        P(None, "head"),
        P(None, "head"),
        P("head", None),
    )
    out_specs = (
        P(SEQ, None),
        P(SEQ, None),
        P(SEQ),
        P(SEQ),
        P(SEQ, "head"),
        P(SEQ, "head"),
        P(SEQ, "head"),
        P(SEQ, "head"),
        P("head", SEQ),
        P(SEQ),
        P(SEQ),
        P(SEQ, "head"),
        P(SEQ, "head"),
        P("head", SEQ),
    )

    def step(*args):
        return shards(*args)

    step = jax.shard_map(step, mesh=mesh, in_specs=in_specs, out_specs=out_specs, check_vma=False)
    return step
```

```python
import functools

import jax
import jax.numpy as jnp
from jax import lax
from jax.experimental import pallas as pl
from jax.experimental.pallas import tpu as pltpu
from jax.sharding import Mesh
from jax.sharding import PartitionSpec as P


KD = 256
VD = 512
SEQ = ("outer", "pair")
PARTS = 4

EPSILON = 1e-05
F32 = jnp.float32
BF16 = jnp.bfloat16
FULL_ACCURACY = lax.Precision.HIGHEST


def after(x, *events):
    return lax.optimization_barrier((x, *events))[0]


def widen(x):
    return lax.reduce_precision(x.astype(F32), 8, 7)


def narrow(x, zero):
    return (x + zero).astype(BF16)


def flip(x, axis, bit):
    count = lax.axis_size(axis)
    return lax.ppermute(x, axis, [(i, i ^ bit) for i in range(count)])


def bits_of(count):
    bits = []
    while (1 << len(bits)) < count:
        bits.append(1 << len(bits))
    assert (1 << len(bits)) == count
    return bits


def relative_order(count):
    order = [0]
    for bit in reversed(bits_of(count)):
        order = order + [j | bit for j in order]
    return order


def to_relative(x, axis_name, dim):
    count, own = lax.axis_size(axis_name), lax.axis_index(axis_name)
    size = x.shape[dim] // count
    return jnp.concatenate(
        [lax.dynamic_slice_in_dim(x, (own ^ j) * size, size, dim) for j in relative_order(count)],
        axis=dim,
    )


def from_relative(x, axis_name, dim):
    count, own = lax.axis_size(axis_name), lax.axis_index(axis_name)
    size = x.shape[dim] // count
    bits = bits_of(count)
    parts = []
    for i in range(count):
        j = own ^ i
        place = 0
        for n in range(len(bits)):
            place = place + ((j >> n) & 1) * (count >> (n + 1))
        parts.append(lax.dynamic_slice_in_dim(x, place * size, size, dim))
    return jnp.concatenate(parts, axis=dim)


def scatter_rows(x, axis_name):
    for bit in bits_of(lax.axis_size(axis_name)):
        half = x.shape[0] // 2
        x = x[:half] + flip(x[half:], axis_name, bit)
    return x


def gather_rows(x, axis_name):
    for bit in reversed(bits_of(lax.axis_size(axis_name))):
        x = jnp.concatenate([x, flip(x, axis_name, bit)], axis=0)
    return x


def layer_norm(values, scales, shifts):
    centred = values - jnp.mean(values, axis=-1, keepdims=True)
    inverse = lax.rsqrt(jnp.mean(centred * centred, axis=-1, keepdims=True) + EPSILON)
    normed = centred * inverse
    return (normed * scales + shifts, normed, inverse)


def norm_back(upstream, normed, inverse):
    return inverse * (
        upstream
        - jnp.mean(upstream, axis=-1, keepdims=True)
        - normed * jnp.mean(upstream * normed, axis=-1, keepdims=True)
    )


def gelu_pair(pre_act):
    normal_cdf = 0.5 * (1.0 + lax.erf(pre_act * 0.7071067811865476))
    density = jnp.exp(-0.5 * pre_act * pre_act) * 0.3989422804014327
    return (pre_act * normal_cdf, normal_cdf + pre_act * density)


def dot(a, b):
    return jnp.dot(a, b, preferred_element_type=F32)


def contract_rows(left_side, right_side, precision=None):
    return lax.dot_general(
        left_side,
        right_side,
        (((0,), (0,)), ((), ())),
        precision=precision,
        preferred_element_type=F32,
    )


def times_transpose(left_side, right_side, precision=None):
    return lax.dot_general(
        left_side,
        right_side,
        (((1,), (1,)), ((), ())),
        precision=precision,
        preferred_element_type=F32,
    )


def carry_states(local, decay, suffix, event=None):
    pairs, odd = lax.axis_size("outer"), lax.axis_index("pair")
    if suffix:
        odd = 1 - odd
    half = local.shape[1] // 2
    keep = lax.dynamic_slice_in_dim(local, odd * half, half, 1)
    give = lax.dynamic_slice_in_dim(local, (1 - odd) * half, half, 1)
    got = flip(give, "pair", 1)
    if event is not None:
        got = after(got, event)
    earlier = jnp.where(odd == 0, keep, got)
    later = jnp.where(odd == 0, got, keep)
    step = decay[:, None, None]
    total = step * earlier + later

    arriving = jnp.zeros_like(total)
    for hop in range(pairs - 1):
        way = (pairs - 1 - hop, pairs - 2 - hop) if suffix else (hop, hop + 1)
        leaving = step * step * arriving + total if hop else total
        arriving = arriving + lax.ppermute(leaving, "outer", [way])
    second = step * arriving + earlier
    mine = jnp.where(odd == 0, arriving, second)
    other = jnp.where(odd == 0, second, arriving)
    rest = flip(other, "pair", 1)
    return jnp.where(
        odd == 0,
        jnp.concatenate([mine, rest], axis=1),
        jnp.concatenate([rest, mine], axis=1),
    )


def scan_kernel(
    pairs,
    pieces,
    decay_ref,
    rate_ref,
    local_ref,
    act_ref,
    gate_weight_ref,
    query_ref,
    key_ref,
    value_ref,
    cot_ref,
    state_ref,
    gate_ref,
    weights_ref,
    intra_ref,
    cot_give_ref,
    got,
    arriving,
    leaving,
    other,
    rest,
    give_send,
    give_recv,
    chain_send,
    chain_recv,
    rest_send,
    rest_recv,
):
    heads, rows, _ = local_ref.shape
    half = rows // 2
    count = heads * pieces
    size = half // pieces
    outer, odd = lax.axis_index("outer"), lax.axis_index("pair")
    is_odd = odd == 1
    has_earlier, has_later = outer > 0, outer < pairs - 1
    partner = {"pair": 1 - odd}

    barrier = pltpu.get_barrier_semaphore()
    pl.semaphore_signal(barrier, device_id=partner, device_id_type=pl.DeviceIdType.MESH)

    @pl.when(has_earlier)
    def _():
        pl.semaphore_signal(
            barrier, device_id={"outer": outer - 1}, device_id_type=pl.DeviceIdType.MESH
        )

    pl.semaphore_wait(barrier, jnp.where(has_later, 2, 1))

    def rows_of(i, which):
        start = which * half + (i % pieces) * size
        return i // pieces, pl.ds(pl.multiple_of(start, size), size)

    def give(i):
        head, place = rows_of(i, 1 - odd)
        return pltpu.make_async_remote_copy(
            src_ref=local_ref.at[head, place],
            dst_ref=got.at[i],
            send_sem=give_send.at[i],
            recv_sem=give_recv.at[i],
            device_id=partner,
            device_id_type=pl.DeviceIdType.MESH,
        )

    def onward(i):
        return pltpu.make_async_remote_copy(
            src_ref=leaving.at[i],
            dst_ref=arriving.at[i],
            send_sem=chain_send.at[i],
            recv_sem=chain_recv.at[i],
            device_id={"outer": outer + 1},
            device_id_type=pl.DeviceIdType.MESH,
        )

    def finish(i):
        return pltpu.make_async_remote_copy(
            src_ref=other.at[i],
            dst_ref=rest.at[i],
            send_sem=rest_send.at[i],
            recv_sem=rest_recv.at[i],
            device_id=partner,
            device_id_type=pl.DeviceIdType.MESH,
        )

    for i in range(count):
        give(i).start()

    columns = gate_weight_ref.shape[1]
    tile = columns // 4

    def gate_tile(n):
        place = pl.ds(n * tile, tile)
        gate_ref[:, place] = jnp.dot(
            act_ref[...], gate_weight_ref[:, place], preferred_element_type=F32
        )

    def scores(h):
        q = query_ref[:, h * KD : (h + 1) * KD]
        k = key_ref[:, h * KD : (h + 1) * KD]
        length = q.shape[0]
        value = times_transpose(q, k)
        place = lax.broadcasted_iota(jnp.int32, (length, length), 0)
        place = place - lax.broadcasted_iota(jnp.int32, (length, length), 1)
        fading = jnp.exp(-rate_ref[h] * jnp.maximum(place, 0).astype(F32))
        weights_ref[h] = jnp.where(place >= 0, value * fading, 0.0).astype(BF16)

    def intra(h):
        intra_ref[h] = jnp.dot(
            weights_ref[h], value_ref[:, h * VD : (h + 1) * VD], preferred_element_type=F32
        )

    def cot_columns():
        block = cot_ref.shape[1] // (2 * pairs)
        count, own = lax.axis_size("head"), lax.axis_index("head")
        part = cot_ref.shape[0] // count
        for place, j in enumerate(relative_order(count)):
            source = pl.ds(pl.multiple_of((own ^ j) * part, part), part)
            for o in range(pairs):
                even = cot_ref[source, pl.ds(2 * o * block, block)]
                uneven = cot_ref[source, pl.ds((2 * o + 1) * block, block)]
                cot_give_ref[pl.ds(place * part, part), pl.ds(o * block, block)] = jnp.where(
                    is_odd, even.astype(F32), uneven.astype(F32)
                )

    work = [functools.partial(gate_tile, n) for n in range(4)] + [cot_columns]
    for h in range(heads):
        work.append(functools.partial(scores, h))
        work.append(functools.partial(intra, h))
    per_piece = -(-(len(work) - 2) // count)
    for job in work[:2]:
        job()
    work = work[2:]

    for i in range(count):
        head, kept_rows = rows_of(i, odd)
        give(i).wait_recv()
        kept, came = local_ref[head, kept_rows], got[i]
        earlier = jnp.where(is_odd, came, kept)
        later = jnp.where(is_odd, kept, came)
        decay = decay_ref[head]

        @pl.when(has_earlier)
        def _():
            onward(i).wait_recv()

        @pl.when(jnp.logical_not(has_earlier))
        def _():
            arriving[i] = jnp.zeros_like(came)

        state = arriving[i]
        second = decay * state + earlier

        @pl.when(has_later)
        def _():
            leaving[i] = decay * second + later
            onward(i).start()

        other[i] = jnp.where(is_odd, state, second)
        finish(i).start()
        state_ref[head, kept_rows] = jnp.where(is_odd, second, state)
        for job in work[:per_piece]:
            job()
        work = work[per_piece:]
    for i in range(count):
        head, place = rows_of(i, 1 - odd)
        finish(i).wait_recv()
        state_ref[head, place] = rest[i]
    for i in range(count):
        give(i).wait_send()
        finish(i).wait_send()

        @pl.when(has_later)
        def _():
            onward(i).wait_send()


def scan_states(local, decay, rate, act, gate_weight, queries, key_rows, value_rows, cotangent):
    heads, rows, columns = local.shape
    length = act.shape[0]
    pieces = 4
    count = heads * pieces
    buffer = pltpu.VMEM((count, rows // 2 // pieces, columns), F32)
    vector = pl.BlockSpec(memory_space=pltpu.VMEM)
    scalar = pl.BlockSpec(memory_space=pltpu.SMEM)
    return pl.pallas_call(
        functools.partial(scan_kernel, lax.axis_size("outer"), pieces),
        out_shape=(
            jax.ShapeDtypeStruct(local.shape, F32),
            jax.ShapeDtypeStruct((length, gate_weight.shape[1]), F32),
            jax.ShapeDtypeStruct((heads, length, length), BF16),
            jax.ShapeDtypeStruct((heads, length, VD), F32),
            jax.ShapeDtypeStruct((length, act.shape[1] // 2), F32),
        ),
        in_specs=[scalar, scalar] + [vector] * 7,
        out_specs=(vector,) * 5,
        scratch_shapes=[buffer] * 5 + [pltpu.SemaphoreType.DMA((count,))] * 6,
        compiler_params=pltpu.CompilerParams(
            collective_id=0, has_side_effects=True, vmem_limit_bytes=40 * 1024 * 1024
        ),
        cost_estimate=pl.CostEstimate(
            flops=2 * length * act.shape[1] * gate_weight.shape[1],
            bytes_accessed=16 * 1024 * 1024,
            transcendentals=heads * length * length,
        ),
    )(decay, rate, local, act, gate_weight, queries, key_rows, value_rows, cotangent)


def mix_kernel(
    parts,
    outer_count,
    gated_ref,
    weight_ref,
    input_ref,
    scale_ref,
    shift_ref,
    up_weight_ref,
    mlp_weight_ref,
    cot_ref,
    down_weight_ref,
    hidden_ref,
    act_ref,
    grads_ref,
    product_ref,
    product_came_ref,
    second_came_ref,
    picked,
    give,
    keep,
    came,
    half,
    landed,
    sent,
    gathered,
    others,
    units,
    product_grad,
    second_give,
    second_came,
    product_give,
    product_came,
    send_sem,
    recv_sem,
):
    own, odd = lax.axis_index("head"), lax.axis_index("pair")
    rows = hidden_ref.shape[0]
    size = rows // parts
    near, far, partner = {"head": own ^ 1}, {"head": own ^ 2}, {"pair": 1 - odd}

    barrier = pltpu.get_barrier_semaphore()
    for device in (near, far, partner):
        pl.semaphore_signal(barrier, device_id=device, device_id_type=pl.DeviceIdType.MESH)
    pl.semaphore_wait(barrier, 3)

    def copy(kind, n, source, target, device):
        return pltpu.make_async_remote_copy(
            src_ref=source,
            dst_ref=target,
            send_sem=send_sem.at[kind, n],
            recv_sem=recv_sem.at[kind, n],
            device_id=device,
            device_id_type=pl.DeviceIdType.MESH,
        )

    def first(n):
        return copy(0, n, give.at[n], came.at[n], near)

    def second(n):
        return copy(1, n, half.at[n], landed.at[n], far)

    def spread_far(n):
        return copy(2, n, sent.at[n], gathered.at[n], far)

    def spread_near(n):
        return copy(3, n, sent.at[n], others.at[n, pl.ds(0, size)], near)

    def forward(n):
        return copy(4, n, gathered.at[n], others.at[n, pl.ds(size, size)], near)

    def columns(n):
        return copy(5, n, second_give.at[n], second_came.at[n], partner)

    def products(n):
        return copy(6, n, product_give.at[n], product_came.at[n], partner)

    for n in range(parts):
        for place, j in enumerate((1, 3, 0, 2)):
            start = pl.multiple_of((own ^ j) * rows + n * size, size)
            picked[pl.ds(place * size, size)] = gated_ref[pl.ds(start, size), :]
        term = jnp.dot(picked[...], weight_ref[...], preferred_element_type=F32)
        give[n] = term[: 2 * size]
        first(n).start()
        keep[n] = term[2 * size :]
    for n in range(parts):
        first(n).wait_recv()
        half[n] = keep[n, pl.ds(size, size)] + came[n, pl.ds(size, size)]
        second(n).start()
    tile = product_grad.shape[1] // 4
    for n in range(4):
        place = pl.ds(n * tile, tile)
        product_grad[:, place] = times_transpose(cot_ref[...], down_weight_ref[place, :])
    block = scale_ref.shape[1] // (2 * outer_count)
    for n in range(parts):
        second(n).wait_recv()
        place = pl.ds(n * size, size)
        hidden = input_ref[place] + (
            keep[n, pl.ds(0, size)] + came[n, pl.ds(0, size)] + landed[n]
        )
        hidden_ref[place] = hidden
        act = layer_norm(hidden, scale_ref[...], shift_ref[...])[0].astype(BF16)
        sent[n] = act.astype(F32)
        spread_far(n).start()
        spread_near(n).start()
        act_ref[place] = act
        for o in range(outer_count):
            second_give[n, :, pl.ds(o * block, block)] = jnp.where(
                odd == 1,
                sent[n, :, pl.ds(2 * o * block, block)],
                sent[n, :, pl.ds((2 * o + 1) * block, block)],
            )
        columns(n).start()
    hidden_units = up_weight_ref.shape[1]
    ups, gates = pl.ds(0, hidden_units), pl.ds(hidden_units, hidden_units)
    for n in range(parts):
        spread_far(n).wait_recv()
        forward(n).start()
        units[pl.ds(0, size)] = act_ref[pl.ds(n * size, size)]
        act = gathered[n].astype(BF16)
        units[pl.ds(size, size)] = act
        act_ref[pl.ds(rows + n * size, size)] = act
        spread_near(n).wait_recv()
        forward(n).wait_recv()
        act = others[n].astype(BF16)
        units[pl.ds(2 * size, 2 * size)] = act
        act_ref[pl.ds(2 * rows + n * size, size)] = act[:size]
        act_ref[pl.ds(3 * rows + n * size, size)] = act[size:]
        mlp_pre = jnp.dot(units[...], mlp_weight_ref[...], preferred_element_type=F32)
        up_pre = jnp.dot(units[...], up_weight_ref[...], preferred_element_type=F32)
        product = (gelu_pair(mlp_pre)[0] * up_pre).astype(BF16)
        product_give[n] = product.astype(F32)
        products(n).start()
        for place in range(4):
            target, source = pl.ds(place * rows + n * size, size), pl.ds(place * size, size)
            product_ref[target] = product[place * size : (place + 1) * size]
            grads_ref[target, ups] = up_pre[place * size : (place + 1) * size]
            grads_ref[target, gates] = mlp_pre[place * size : (place + 1) * size]
    length = grads_ref.shape[0]
    step = length // 8
    for n in range(8):
        place = pl.ds(n * step, step)
        value, slope = gelu_pair(grads_ref[place, gates])
        grad = product_grad[place]
        up_pre = grads_ref[place, ups]
        grads_ref[place, ups] = (grad * value).astype(BF16).astype(F32)
        grads_ref[place, gates] = (grad * up_pre * slope).astype(BF16).astype(F32)
    for n in range(parts):
        columns(n).wait_recv()
        second_came_ref[pl.ds(n * size, size)] = second_came[n]
    for n in range(parts):
        products(n).wait_recv()
        for place in range(4):
            product_came_ref[pl.ds(place * rows + n * size, size)] = product_came[
                n, pl.ds(place * size, size)
            ].astype(BF16)
    for n in range(parts):
        for done in (first, second, spread_far, spread_near, forward, columns, products):
            done(n).wait_send()


def mix_rows(gated, weight, inputs, scale, shift, up_weight, mlp_weight, cotangent, down_weight):
    rows, width = inputs.shape
    count = lax.axis_size("head")
    assert count == 4
    parts = PARTS
    size = rows // parts
    units = up_weight.shape[1]
    length = count * rows

    def buffer(*shape, dtype=F32):
        return pltpu.VMEM(shape, dtype)

    vector = pl.BlockSpec(memory_space=pltpu.VMEM)
    return pl.pallas_call(
        functools.partial(mix_kernel, parts, lax.axis_size("outer")),
        out_shape=(
            jax.ShapeDtypeStruct((rows, width), F32),
            jax.ShapeDtypeStruct((length, width), BF16),
            jax.ShapeDtypeStruct((length, 2 * units), F32),
            jax.ShapeDtypeStruct((length, units), BF16),
            jax.ShapeDtypeStruct((length, units), BF16),
            jax.ShapeDtypeStruct((rows, width // 2), F32),
        ),
        in_specs=[vector] * 9,
        out_specs=(vector,) * 6,
        scratch_shapes=[
            buffer(4 * size, gated.shape[1], dtype=BF16),
            buffer(parts, 2 * size, width),
            buffer(parts, 2 * size, width),
            buffer(parts, 2 * size, width),
            buffer(parts, size, width),
            buffer(parts, size, width),
            buffer(parts, size, width),
            buffer(parts, size, width),
            buffer(parts, 2 * size, width),
            buffer(4 * size, width, dtype=BF16),
            buffer(length, units),
            buffer(parts, size, width // 2),
            buffer(parts, size, width // 2),
            buffer(parts, 4 * size, units),
            buffer(parts, 4 * size, units),
            pltpu.SemaphoreType.DMA((7, parts)),
            pltpu.SemaphoreType.DMA((7, parts)),
        ],
        compiler_params=pltpu.CompilerParams(
            collective_id=1, has_side_effects=True, vmem_limit_bytes=62 * 1024 * 1024
        ),
        cost_estimate=pl.CostEstimate(
            flops=2 * length * width * (gated.shape[1] + 3 * units),
            bytes_accessed=100 * 1024 * 1024,
            transcendentals=0,
        ),
    )(
        gated,
        weight,
        inputs,
        scale[None],
        shift[None],
        up_weight,
        mlp_weight,
        cotangent,
        down_weight,
    )


def split_columns(x):
    outer, place = lax.axis_size("outer"), lax.axis_index("pair")
    size = x.shape[1] // (2 * outer)

    def blocks(which):
        return jnp.concatenate(
            [lax.dynamic_slice_in_dim(x, (2 * o + which) * size, size, 1) for o in range(outer)],
            axis=1,
        )

    return blocks(place), blocks(1 - place)


def sum_blocks(x):
    return lax.psum_scatter(x, "outer", scatter_dimension=0, tiled=True)


def shards(
    block_input,
    out_cotangent,
    decay_rate,
    first_scale,
    first_shift,
    query_weight,
    key_weight,
    value_weight,
    gate_weight,
    output_weight,
    second_scale,
    second_shift,
    up_weight,
    mlp_gate_weight,
    down_weight,
):
    length, _ = block_input.shape
    local_heads = decay_rate.shape[0]
    head_range = range(local_heads)
    zero = decay_rate[0] * 0.0

    places = jnp.arange(length, dtype=F32)
    distance = places[:, None] - places[None, :]
    causal = distance >= 0.0
    safe = jnp.where(causal, distance, 0.0)
    masks = [jnp.where(causal, jnp.exp(-decay_rate[h] * safe), 0.0) for h in head_range]
    fade_in = [jnp.exp(-places * decay_rate[h])[:, None] for h in head_range]
    fade_out = [jnp.exp(-(length - places) * decay_rate[h])[:, None] for h in head_range]
    block_decay = jnp.exp(-decay_rate * length)

    inputs = block_input.astype(F32)
    first_out, first_normed, first_inverse = layer_norm(inputs, first_scale, first_shift)
    first_act = first_out.astype(BF16)
    queries = dot(first_act, query_weight).astype(BF16)
    key_rows = dot(first_act, key_weight).astype(BF16)
    value_rows = dot(first_act, value_weight).astype(BF16)
    q = [queries[:, h * KD : (h + 1) * KD] for h in head_range]
    k = [key_rows[:, h * KD : (h + 1) * KD] for h in head_range]
    v = [value_rows[:, h * VD : (h + 1) * VD] for h in head_range]
    local_state = jnp.stack(
        [
            contract_rows(k[h].astype(F32) * fade_out[h], v[h].astype(F32), FULL_ACCURACY)
            for h in head_range
        ]
    )
    state_in, gate_pre, retain_weights, intra, cot_given = scan_states(
        local_state,
        block_decay,
        decay_rate,
        first_act,
        gate_weight,
        queries,
        key_rows,
        value_rows,
        out_cotangent,
    )

    sigmoid_gate = jax.nn.sigmoid(gate_pre)
    swish_gate = gate_pre * sigmoid_gate
    group_normed, spread = [], []
    for h in head_range:
        retained = intra[h] + fade_in[h] * jnp.dot(
            q[h].astype(F32), state_in[h], precision=FULL_ACCURACY
        )
        centred = retained - jnp.mean(retained, axis=-1, keepdims=True)
        inverse = lax.rsqrt(jnp.mean(centred * centred, axis=-1, keepdims=True) + EPSILON)
        group_normed.append(centred * inverse)
        spread.append(inverse)
    gated_rows = jnp.concatenate(
        [swish_gate[:, h * VD : (h + 1) * VD] * group_normed[h] for h in head_range], axis=1
    ).astype(BF16)
    own_rows = length // lax.axis_size("head")
    row_start = lax.axis_index("head") * own_rows
    input_rows = lax.dynamic_slice_in_dim(block_input, row_start, own_rows, 0).astype(F32)
    cot_rows = lax.dynamic_slice_in_dim(out_cotangent, row_start, own_rows, 0).astype(F32)

    cot_rel = to_relative(out_cotangent, "head", 0)
    cot_came = narrow(flip(cot_given, "pair", 1), zero)

    hidden, second_act, mlp_wide, product, product_came, second_given = mix_rows(
        gated_rows,
        output_weight,
        input_rows,
        second_scale,
        second_shift,
        up_weight,
        mlp_gate_weight,
        cot_rel,
        down_weight,
    )
    _, second_normed, second_inverse = layer_norm(hidden, second_scale, second_shift)
    first_kept, first_given = split_columns(first_act)
    first_given = flip(after(widen(first_given), hidden), "pair", 1)

    mlp_given = flip(mlp_wide, "pair", 1)

    cot_pair = jnp.concatenate([split_columns(cot_rel)[0], cot_came])
    product_pair = jnp.concatenate([product, product_came])
    down_term = contract_rows(cot_pair, product_pair)
    down_grad = sum_blocks(down_term).T

    mlp_grads = after(mlp_wide, down_term).astype(BF16)
    hidden_units = up_weight.shape[1]
    up_pre_grad, mlp_pre_grad = mlp_grads[:, :hidden_units], mlp_grads[:, hidden_units:]
    second_act_grad = times_transpose(up_pre_grad, up_weight) + times_transpose(
        mlp_pre_grad, mlp_gate_weight
    )
    second_act_grad = scatter_rows(second_act_grad, "head")
    hidden_grad = cot_rows + norm_back(
        second_act_grad * second_scale, second_normed, second_inverse
    )
    cast_rows = widen(hidden_grad)
    cast_all = gather_rows(cast_rows, "head")


    second_given = narrow(gather_rows(second_given, "head"), zero)
    second_pair = jnp.concatenate([split_columns(second_act)[0], second_given])
    mlp_pair = jnp.concatenate([mlp_grads, narrow(mlp_given, zero)])
    mlp_term = contract_rows(second_pair, mlp_pair)
    mlp_both = sum_blocks(mlp_term)
    up_grad, mlp_gate_grad = mlp_both[:, :hidden_units], mlp_both[:, hidden_units:]
    hidden_cast = from_relative(narrow(after(cast_all, mlp_term), zero), "head", 0)
    gated_grad = times_transpose(hidden_cast, output_weight)
    group_flat = jnp.concatenate(group_normed, axis=1)
    gate_pre_grad = (
        gated_grad * group_flat * sigmoid_gate * (1.0 + gate_pre * (1.0 - sigmoid_gate))
    ).astype(BF16)
    normed_grad = gated_grad * swish_gate
    retained_grad = [
        norm_back(normed_grad[:, h * VD : (h + 1) * VD], group_normed[h], spread[h]).astype(BF16)
        for h in head_range
    ]
    state_term = jnp.stack(
        [
            contract_rows(
                q[h].astype(F32) * fade_in[h], retained_grad[h].astype(F32), FULL_ACCURACY
            )
            for h in head_range
        ]
    )
    cast_given = flip(split_columns(cast_rows)[1], "pair", 1)
    gated_given = flip(after(widen(gated_rows), cast_rows), "pair", 1)
    gate_given = flip(widen(gate_pre_grad), "pair", 1)

    state_grad = carry_states(state_term, block_decay, True, mlp_term)

    output_rows = hidden + scatter_rows(dot(product, after(down_weight, cast_rows)), "head")
    output_rows = widen(output_rows)
    block_output = from_relative(narrow(gather_rows(output_rows, "head"), zero), "head", 0)

    second_scale_part = jnp.sum(second_act_grad * second_normed, axis=0)
    second_shift_part = jnp.sum(second_act_grad, axis=0)

    query_parts, key_parts, value_parts = [], [], []
    for h in head_range:
        score_grad = (times_transpose(retained_grad[h], v[h]) * masks[h]).astype(BF16)
        query_parts.append(
            dot(score_grad, k[h])
            + fade_in[h]
            * times_transpose(retained_grad[h].astype(F32), state_in[h], FULL_ACCURACY)
        )
        key_parts.append(
            contract_rows(score_grad, q[h])
            + fade_out[h] * times_transpose(v[h].astype(F32), state_grad[h], FULL_ACCURACY)
        )
        value_parts.append(
            contract_rows(retain_weights[h], retained_grad[h])
            + fade_out[h]
            * jnp.dot(k[h].astype(F32), state_grad[h], precision=FULL_ACCURACY)
        )
    head_grads = jnp.concatenate(query_parts + key_parts + value_parts, axis=1).astype(BF16)
    head_given = flip(widen(head_grads), "pair", 1)

    cast_given = from_relative(narrow(gather_rows(cast_given, "head"), zero), "head", 0)
    cast_pair = jnp.concatenate([split_columns(hidden_cast)[0], cast_given])
    gated_pair = jnp.concatenate([gated_rows, narrow(gated_given, zero)])
    first_pair = jnp.concatenate([first_kept, narrow(first_given, zero)])
    gate_pair = jnp.concatenate([gate_pre_grad, narrow(gate_given, zero)])
    output_term = jnp.concatenate(
        [contract_rows(cast_pair, gated_pair), contract_rows(first_pair, gate_pair)], axis=1
    )
    output_both = sum_blocks(output_term)
    output_columns = gated_rows.shape[1]
    output_grad, gate_grad = output_both[:, :output_columns].T, output_both[:, output_columns:]

    head_pair = jnp.concatenate([head_grads, narrow(after(head_given, output_term), zero)])
    head_both = sum_blocks(contract_rows(first_pair, head_pair))
    key_columns, value_columns = local_heads * KD, 2 * local_heads * KD
    query_grad = head_both[:, :key_columns]
    key_grad = head_both[:, key_columns:value_columns]
    value_grad = head_both[:, value_columns:]

    first_act_grad = (
        times_transpose(head_grads[:, :key_columns], query_weight)
        + times_transpose(head_grads[:, key_columns:value_columns], key_weight)
        + times_transpose(head_grads[:, value_columns:], value_weight)
        + times_transpose(gate_pre_grad, gate_weight)
    )
    first_act_grad = scatter_rows(to_relative(first_act_grad, "head", 0), "head")
    normed_rows = lax.dynamic_slice_in_dim(first_normed, row_start, own_rows, 0)
    inverse_rows = lax.dynamic_slice_in_dim(first_inverse, row_start, own_rows, 0)
    first_scale_part = jnp.sum(first_act_grad * normed_rows, axis=0)
    first_shift_part = jnp.sum(first_act_grad, axis=0)
    grad_rows = hidden_grad + norm_back(first_act_grad * first_scale, normed_rows, inverse_rows)
    grad_rows = widen(grad_rows)
    input_grad = from_relative(narrow(gather_rows(grad_rows, "head"), zero), "head", 0)

    vectors = jnp.stack([first_scale_part, first_shift_part, second_scale_part, second_shift_part])
    kept, given = split_columns(vectors)
    vectors = kept + flip(given, "pair", 1)
    vectors = to_relative(vectors, "outer", 1)
    for bit in bits_of(lax.axis_size("outer")):
        half = vectors.shape[1] // 2
        vectors = vectors[:, :half] + flip(vectors[:, half:], "outer", bit)
    for bit in bits_of(lax.axis_size("head")):
        vectors = vectors + flip(vectors, "head", bit)
    return (
        block_output,
        input_grad,
        vectors[0],
        vectors[1],
        query_grad,
        key_grad,
        value_grad,
        gate_grad,
        output_grad,
        vectors[2],
        vectors[3],
        up_grad,
        mlp_gate_grad,
        down_grad,
    )


def solution(mesh):
    seq, head = mesh.shape["seq"], mesh.shape["head"]
    mesh = Mesh(mesh.devices.reshape(seq // 2, 2, head), ("outer", "pair", "head"))
    in_specs = (
        P(SEQ, None),
        P(SEQ, None),
        P("head"),
        P(),
        P(),
        P(None, "head"),
        P(None, "head"),
        P(None, "head"),
        P(None, "head"),
        P("head", None),
        P(),
        P(),
        P(None, "head"),
        P(None, "head"),
        P("head", None),
    )
    out_specs = (
        P(SEQ, None),
        P(SEQ, None),
        P(SEQ),
        P(SEQ),
        P(SEQ, "head"),
        P(SEQ, "head"),
        P(SEQ, "head"),
        P(SEQ, "head"),
        P("head", SEQ),
        P(SEQ),
        P(SEQ),
        P(SEQ, "head"),
        P(SEQ, "head"),
        P("head", SEQ),
    )

    def step(*args):
        return shards(*args)

    step = jax.shard_map(step, mesh=mesh, in_specs=in_specs, out_specs=out_specs, check_vma=False)
    return step
```
